32 devices in a mesh: dp: 4 (over x, core), ctx: 8 (over z, y).
Axes of the slice: x: 2, y: 2, z: 4, core: 2. Of those that a mesh axis runs over, the one named last changes fastest.
Arguments:
- density: float32 [128, 64, 64], P(('dp', 'ctx')), parts along dimension 0, may hold values from 0.1 to 50, as said below
- stem_weight: bfloat16 [216, 1024], replicated, may hold values from -0.4375 to 0.4375
- stem_bias: float32 [1024], replicated, may hold values from -3 to 3
- pos_embed: bfloat16 [2048, 1024], P('ctx'), may hold values from -3 to 3
- ln1_gain: float32 [1024], replicated, may hold values from 0.25 to 1.75
- ln1_bias: float32 [1024], replicated, may hold values from -2 to 2
- w_qkv: bfloat16 [1024, 3072], replicated, may hold values from -2 to 2
- qkv_bias: float32 [3072], replicated, may hold values from -2 to 2
- w_out: bfloat16 [1024, 1024], replicated, may hold values from -0.1875 to 0.1875
- out_bias: float32 [1024], replicated, may hold values from -2 to 2
- ln2_gain: float32 [1024], replicated, may hold values from 0.25 to 1.75
- ln2_bias: float32 [1024], replicated, may hold values from -2 to 2
- w_fc1: bfloat16 [1024, 4096], replicated, may hold values from -0.1875 to 0.1875
- fc1_bias: float32 [4096], replicated, may hold values from -3 to 3
- w_fc2: bfloat16 [4096, 1024], replicated, may hold values from -0.09375 to 0.09375
- fc2_bias: float32 [1024], replicated, may hold values from -2 to 2
Outputs:
- encoded: bfloat16 [8192, 1024], P(('dp', 'ctx')), parts along dimension 0
The draws below stay inside these ranges and needn't reach their ends.
There are 4 independent parts, one for each index of `dp`. The reference program is written for one: setup_inputs(seed, part) draws one part's arguments, and reference() takes and returns one part's arrays. A program takes and returns all parts, laid end to end along the dimension named above; an argument that names none is the same for every part. Nothing has to cross between parts.
Inputs may be any that keep to these rules, and one draw needn't show every extreme that they name: density is positive.
All inputs are finite; a program needn't handle non-finite values.
Results may differ from the reference program's by a relative error of at most 0.013.
Values may be sent and summed in bfloat16 or wider, within the bound.
A program may use at most 384 MiB of HBM per device.

```python
import math
import jax
import jax.numpy as jnp
from jax import lax

D = 1024
FF = 4096
HEADS = 16
KERNEL = 6
STRIDE = 4
GYZ = 16
TX = 8
TOKENS = 2048


def draw_density(key, part):
    planes = STRIDE * TX
    side_cells = STRIDE * GYZ
    key_one = jax.random.fold_in(key, 11)
    gradient = jnp.arange(planes, dtype=jnp.float32)[:, None, None] / max(planes - 1, 1)
    entries = jnp.exp(jax.random.uniform(key_one, (planes, side_cells, side_cells), jnp.float32, math.log(0.2), math.log(5.0)))
    scaling = jnp.exp(math.log(3.0) * gradient)
    return entries * scaling


def draw_w_qkv(key, part):
    key_one = jax.random.fold_in(jax.random.fold_in(key, 23), 0)
    spread = 1.6 / math.sqrt(D)
    return (jnp.clip(jax.random.normal(key_one, (D, 3 * D), jnp.float32), -6.0, 6.0) * spread).astype(jnp.bfloat16)


def block_scale(stream_key, extent, shards, low, top_value):
    def one(position, parts):
        draws = jax.random.uniform(jax.random.fold_in(jax.random.fold_in(stream_key, 6), position), (parts,), jnp.float32, low / len(shards), top_value / len(shards))
        return jnp.repeat(jnp.exp(draws), extent[position] // parts).reshape((-1,) + (1,) * (len(extent) - position - 1))

    level = one(*shards[0])
    for cut in shards[1:]:
        level = level * one(*cut)
    return level


def scatter_about(key, extent, scale, most, cuts=(), kind=jnp.bfloat16):
    gain = block_scale(key, extent, cuts, -0.22, 0.18) if cuts else 1.0
    values = jax.random.normal(key, extent, jnp.float32) * scale * gain
    return jnp.minimum(jnp.maximum(values, -most), most).astype(kind)


def setup_inputs(seed: int = 0, part: int = 0) -> dict:
    key_list = jax.random.split(jax.random.key(seed), 17)
    part_keys = jax.random.split(jax.random.fold_in(key_list[16], part), 17)
    return {
        "density": draw_density(jax.random.fold_in(jax.random.fold_in(key_list[16], part), 71), part),
        "stem_weight": scatter_about(key_list[1], (KERNEL * KERNEL * KERNEL, D), (KERNEL * KERNEL * KERNEL) ** -0.5, 0.4375),
        "stem_bias": scatter_about(key_list[2], (D,), 0.5, 3.0, (), jnp.float32),
        "pos_embed": scatter_about(key_list[3], (TOKENS, D), 0.5, 3.0, ((0, 8),)),
        "ln1_gain": jnp.clip(1.0 + 0.15 * jax.random.normal(key_list[4], (D,), jnp.float32), 0.25, 1.75),
        "ln1_bias": scatter_about(key_list[5], (D,), 0.3, 2.0, (), jnp.float32),
        "w_qkv": draw_w_qkv(jax.random.fold_in(key_list[16], 71), part),
        "qkv_bias": scatter_about(key_list[7], (3 * D,), 0.3, 2.0, (), jnp.float32),
        "w_out": scatter_about(key_list[8], (D, D), D ** -0.5, 0.1875),
        "out_bias": scatter_about(key_list[9], (D,), 0.3, 2.0, (), jnp.float32),
        "ln2_gain": jnp.clip(1.0 + 0.15 * jax.random.normal(key_list[10], (D,), jnp.float32), 0.25, 1.75),
        "ln2_bias": scatter_about(key_list[11], (D,), 0.3, 2.0, (), jnp.float32),
        "w_fc1": scatter_about(key_list[12], (D, FF), D ** -0.5, 0.1875),
        "fc1_bias": scatter_about(key_list[13], (FF,), 0.5, 3.0, (), jnp.float32),
        "w_fc2": scatter_about(key_list[14], (FF, D), FF ** -0.5, 0.09375),
        "fc2_bias": scatter_about(key_list[15], (D,), 0.3, 2.0, (), jnp.float32),
    }


def layer_norm(inputs, gain_vector, shift_vector):
    values = inputs.astype(jnp.float32)
    center = values - lax.optimization_barrier(jnp.mean(values, axis=-1, keepdims=True))
    spread = lax.optimization_barrier(jnp.mean(center * center, axis=-1, keepdims=True))
    return center * lax.rsqrt(spread + 1e-06) * gain_vector + shift_vector

def stem_conv(stacked, stem_weight):
    model_width = stem_weight.shape[1]
    kernel = stem_weight.reshape(6, 6, 6, 1, model_width)
    result = lax.conv_general_dilated(stacked[..., None], kernel, (4, 4, 4), ((1, 1), (1, 1), (1, 1)), dimension_numbers=('NDHWC', 'DHWIO', 'NDHWC'), preferred_element_type=jnp.float32)
    return result.reshape(-1, model_width)

def single_head(triple):
    query_head, key_head, value_head = triple
    scores = jnp.dot(query_head, key_head.T, preferred_element_type=jnp.float32)
    row_max = lax.optimization_barrier(jnp.max(scores, axis=1, keepdims=True))
    weights = jnp.exp(scores - row_max)
    row_total = lax.optimization_barrier(jnp.sum(weights, axis=1, keepdims=True))
    mixed = jnp.dot(weights.astype(jnp.bfloat16), value_head, preferred_element_type=jnp.float32) / row_total
    return mixed.astype(jnp.bfloat16)

def reference(density, stem_weight, stem_bias, pos_embed, ln1_gain, ln1_bias, w_qkv, qkv_bias, w_out, out_bias, ln2_gain, ln2_bias, w_fc1, fc1_bias, w_fc2, fc2_bias):
    model_width = w_out.shape[0]
    head_size = model_width // HEADS
    mean_density = jnp.mean(density)
    field = jnp.log(density / mean_density).astype(jnp.bfloat16)
    embedded = stem_conv(field[None], stem_weight) + stem_bias + pos_embed.astype(jnp.float32)
    residual = embedded.astype(jnp.bfloat16)
    normed = layer_norm(residual, ln1_gain, ln1_bias).astype(jnp.bfloat16)
    projected = jnp.dot(normed, w_qkv, preferred_element_type=jnp.float32) + qkv_bias
    token_count = normed.shape[0]
    query_rows = (projected[:, :model_width] * (1.0 / head_size ** 0.5)).astype(jnp.bfloat16)
    key_rows = projected[:, model_width:2 * model_width].astype(jnp.bfloat16)
    value_rows = projected[:, 2 * model_width:].astype(jnp.bfloat16)

    def split_heads(matrix):
        return matrix.reshape(token_count, HEADS, head_size).transpose(1, 0, 2)
    attended = lax.map(single_head, (split_heads(query_rows), split_heads(key_rows), split_heads(value_rows)))
    attended = attended.transpose(1, 0, 2).reshape(token_count, model_width)
    stream = (residual.astype(jnp.float32) + jnp.dot(attended, w_out, preferred_element_type=jnp.float32) + out_bias).astype(jnp.bfloat16)
    normed_two = layer_norm(stream, ln2_gain, ln2_bias).astype(jnp.bfloat16)
    hidden = jax.nn.gelu(jnp.dot(normed_two, w_fc1, preferred_element_type=jnp.float32) + fc1_bias, approximate=False).astype(jnp.bfloat16)
    encoded = stream.astype(jnp.float32) + jnp.dot(hidden, w_fc2, preferred_element_type=jnp.float32) + fc2_bias
    return encoded.astype(jnp.bfloat16)
```

```python
import functools
import math

import jax
import jax.numpy as jnp
from jax import lax
from jax.experimental import pallas as pl
from jax.experimental.pallas import tpu as pltpu
from jax.sharding import PartitionSpec as P

HEADS = 16
KERNEL = 6
STRIDE = 4
MESH = pl.DeviceIdType.MESH
F32 = jnp.float32
BF16 = jnp.bfloat16


def iota(shape, axis):
    return lax.broadcasted_iota(jnp.int32, shape, axis)


def norm_rows(values, gain_vector, shift_vector):
    center = values - jnp.mean(values, axis=-1, keepdims=True)
    spread = jnp.mean(center * center, axis=-1, keepdims=True)
    return center * lax.rsqrt(spread + 1e-06) * gain_vector + shift_vector


def layer_kernel(
    n,
    cells,
    density,
    stem_weight,
    stem_bias,
    pos_embed,
    ln1_gain,
    ln1_bias,
    w_qkv_hbm,
    qkv_bias,
    w_out_hbm,
    out_bias,
    ln2_gain,
    ln2_bias,
    w_fc1_hbm,
    fc1_bias,
    w_fc2_hbm,
    fc2_bias,
    encoded,
    w_qkv,
    w_out,
    w_fc1,
    w_fc2,
    weight_sem,
    halo,
    sum_send,
    sum_got,
    edge_send_sem,
    edge_recv_sem,
    sum_send_sem,
    sum_recv_sem,
    select_rows,
    fold,
    planes_wide,
    kernel_rows,
    residual,
    normed,
    outgoing,
    query_got,
    key_got,
    value_got,
    value_wide,
    mixed_send,
    mixed_got,
    attended,
    total,
    send_sem,
    recv_sem,
):
    me = lax.axis_index("ctx")
    planes, side, _ = density.shape
    tokens, width = residual.shape
    head_size = width // HEADS
    local_heads = max(HEADS // n, 1)
    groups = max(n // HEADS, 1)
    group_width = local_heads * head_size
    share = tokens // groups
    grid = side // STRIDE
    window = planes + 2

    weights = [
        pltpu.make_async_copy(source, target, weight_sem.at[i])
        for i, (source, target) in enumerate(
            ((w_qkv_hbm, w_qkv), (w_out_hbm, w_out), (w_fc1_hbm, w_fc1), (w_fc2_hbm, w_fc2))
        )
    ]
    for copy in weights:
        copy.start()

    barrier = pltpu.get_barrier_semaphore()

    def each_peer(action):
        def step(offset, carry):
            action(lax.rem(me + offset, n))
            return carry

        lax.fori_loop(1, n, step, 0)

    each_peer(
        lambda peer: pl.semaphore_signal(
            barrier, inc=1, device_id={"ctx": peer}, device_id_type=MESH
        )
    )

    own = jnp.sum(density[...], axis=0)
    own = jnp.sum(own, axis=(0, 1), keepdims=True)
    sum_send[...] = jnp.broadcast_to(own, sum_send.shape)
    sum_got[me] = jnp.broadcast_to(own, sum_send.shape)

    @pl.when(me == 0)
    def _():
        halo[0] = jnp.ones((side, side), F32)

    @pl.when(me == n - 1)
    def _():
        halo[1] = jnp.ones((side, side), F32)

    pl.semaphore_wait(barrier, n - 1)

    def edge(side_index, plane, peer):
        return pltpu.make_async_remote_copy(
            src_ref=density.at[plane],
            dst_ref=halo.at[side_index],
            send_sem=edge_send_sem.at[side_index],
            recv_sem=edge_recv_sem.at[side_index],
            device_id={"ctx": peer},
            device_id_type=MESH,
        )

    up = edge(0, planes - 1, lax.rem(me + 1, n))
    down = edge(1, 0, lax.rem(me + n - 1, n))

    def sum_copy(source, peer):
        return pltpu.make_async_remote_copy(
            src_ref=sum_send,
            dst_ref=sum_got.at[source],
            send_sem=sum_send_sem.at[peer],
            recv_sem=sum_recv_sem.at[source],
            device_id={"ctx": peer},
            device_id_type=MESH,
        )

    each_peer(lambda peer: sum_copy(me, peer).start())

    @pl.when(me < n - 1)
    def _():
        up.start()

    @pl.when(me > 0)
    def _():
        down.start()

    pair = 2 * side
    row = iota((tokens, side), 0)
    col = iota((tokens, side), 1)
    for b in range(KERNEL):
        hit = col == STRIDE * (row // grid) - 1 + b
        select_rows[b] = jnp.where(hit, 1.0, 0.0).astype(BF16)
    lane_row = iota((pair, 256), 0)
    lane_col = iota((pair, 256), 1)
    high = lane_row // side
    offset_c = ((lane_row + 1) & (STRIDE - 1)) + STRIDE * high
    for b in range(KERNEL):
        for a in range(window):
            hit = (offset_c < KERNEL) & (lane_col == (a * KERNEL + b) * KERNEL + offset_c)
            fold[b, a * pair : (a + 1) * pair, :] = jnp.where(hit, 1.0, 0.0).astype(BF16)
    taps = stem_weight.shape[0]
    kernel_rows[...] = jnp.zeros(kernel_rows.shape, BF16)
    kernel_rows[0:taps, :] = stem_weight[...]
    tile_row = iota((tokens, pair), 0)
    tile_lane = iota((tokens, pair), 1)
    keep = (((tile_lane & (side - 1)) + 1) // STRIDE - tile_lane // side) == (
        tile_row & (grid - 1)
    )
    keep = jnp.where(keep, 1.0, 0.0).astype(BF16)

    each_peer(lambda peer: sum_copy(peer, peer).wait_recv())

    @pl.when(me > 0)
    def _():
        up.wait_recv()

    @pl.when(me < n - 1)
    def _():
        down.wait_recv()

    mean_density = (jnp.sum(sum_got[...], axis=0)[0:1, 0:1]) / cells
    for a in range(window):
        if a == 0:
            plane = jnp.where(me > 0, jnp.log(halo[0] / mean_density), 0.0)
        elif a == window - 1:
            plane = jnp.where(me < n - 1, jnp.log(halo[1] / mean_density), 0.0)
        else:
            plane = jnp.log(density[a - 1] / mean_density)
        plane = plane.astype(BF16)
        planes_wide[:, a * pair : (a + 1) * pair] = jnp.concatenate([plane, plane], axis=1)

    keep_wide = jnp.concatenate([keep] * window, axis=1)
    patches = jnp.zeros((tokens, 256), F32)
    for b in range(KERNEL):
        rows = jnp.dot(select_rows[b], planes_wide[...], preferred_element_type=F32)
        rows = rows.astype(BF16) * keep_wide
        patches += jnp.dot(rows, fold[b], preferred_element_type=F32)
    embedded = jnp.dot(patches.astype(BF16), kernel_rows[...], preferred_element_type=F32)
    embedded = embedded + stem_bias[...] + pos_embed[...].astype(F32)
    residual[...] = embedded.astype(BF16)
    normed[...] = norm_rows(residual[...].astype(F32), ln1_gain[...], ln1_bias[...]).astype(BF16)

    def head_group(peer):
        return peer // groups

    def my_rows(peer):
        return pl.ds(pl.multiple_of(lax.rem(peer, groups) * share, share), share)

    def projected_copy(kind, source, peer):
        piece = outgoing.at[kind, head_group(peer)]
        got = (query_got, key_got, value_got)[kind]
        if kind == 0:
            piece = piece.at[my_rows(peer)]
        return pltpu.make_async_remote_copy(
            src_ref=piece,
            dst_ref=got.at[source],
            send_sem=send_sem.at[kind, peer],
            recv_sem=recv_sem.at[kind, source],
            device_id={"ctx": peer},
            device_id_type=MESH,
        )

    weights[0].wait()
    block = 256
    for kind in (1, 2, 0):
        for start in range(0, width, block):
            columns = slice(kind * width + start, kind * width + start + block)
            result = jnp.dot(normed[...], w_qkv[:, columns], preferred_element_type=F32)
            result = result + qkv_bias[:, columns]
            if kind == 0:
                result = result * (1.0 / head_size**0.5)
            result = result.astype(BF16)
            for part in range(block // group_width):
                outgoing[kind, start // group_width + part] = result[
                    :, part * group_width : (part + 1) * group_width
                ]
        each_peer(lambda peer: projected_copy(kind, me, peer).start())
    query_got[me] = outgoing[0, head_group(me), my_rows(me), :]
    key_got[me] = outgoing[1, head_group(me)]
    value_got[me] = outgoing[2, head_group(me)]

    each_peer(lambda peer: projected_copy(1, peer, peer).wait_recv())
    each_peer(lambda peer: projected_copy(2, peer, peer).wait_recv())

    keys_total = n * tokens
    wide = group_width % 128 == 0
    if wide:
        value_wide[:, 0:group_width] = value_got[...].reshape(keys_total, group_width)
        value_wide[:, group_width:] = jnp.ones((keys_total, group_width), BF16)

    def mixed_copy(source, peer):
        return pltpu.make_async_remote_copy(
            src_ref=mixed_send.at[peer],
            dst_ref=mixed_got.at[source],
            send_sem=send_sem.at[3, peer],
            recv_sem=recv_sem.at[3, source],
            device_id={"ctx": peer},
            device_id_type=MESH,
        )

    def attend(offset, carry):
        peer = lax.rem(me + n - offset, n)

        @pl.when(offset > 0)
        def _():
            projected_copy(0, peer, peer).wait_recv()

        query = query_got[peer]
        lane = iota((share, group_width), 1) // head_size
        mixed = None
        for head in range(local_heads):
            mine = query if local_heads == 1 else jnp.where(lane == head, query, jnp.zeros_like(query))
            scores = lax.dot_general(
                mine,
                key_got[...].reshape(keys_total, group_width),
                (((1,), (1,)), ((), ())),
                preferred_element_type=F32,
            )
            weight = jnp.exp(scores - jnp.max(scores, axis=1, keepdims=True))
            if wide:
                product = jnp.dot(weight.astype(BF16), value_wide[...], preferred_element_type=F32)
                part = product[:, 0:group_width] / product[:, group_width:]
            else:
                product = jnp.dot(
                    weight.astype(BF16),
                    value_got[...].reshape(keys_total, group_width),
                    preferred_element_type=F32,
                )
                part = product / jnp.sum(weight, axis=1, keepdims=True)
            mixed = part if mixed is None else jnp.where(lane == head, part, mixed)
        mixed_send[peer] = mixed.astype(BF16)

        @pl.when(offset > 0)
        def _():
            mixed_copy(me, peer).start()

        @pl.when(offset == 0)
        def _():
            mixed_got[me] = mixed.astype(BF16)

        return carry

    lax.fori_loop(0, n, attend, 0)

    each_peer(lambda peer: mixed_copy(peer, peer).wait_recv())
    for piece in range(n):
        first = (piece % groups) * share
        column = (piece // groups) * group_width
        attended[first : first + share, column : column + group_width] = mixed_got[piece]

    weights[1].wait()
    stream = (
        residual[...].astype(F32)
        + jnp.dot(attended[...], w_out[...], preferred_element_type=F32)
        + out_bias[...]
    ).astype(BF16)
    residual[...] = stream
    stream = stream.astype(F32)
    normed[...] = norm_rows(stream, ln2_gain[...], ln2_bias[...]).astype(BF16)
    total[...] = stream + fc2_bias[...]

    weights[2].wait()
    weights[3].wait()
    hidden_width = w_fc1.shape[1]
    tile = math.gcd(hidden_width, 512)
    for start in range(0, hidden_width, tile):
        columns = slice(start, start + tile)
        hidden = jnp.dot(normed[...], w_fc1[:, columns], preferred_element_type=F32)
        hidden = hidden + fc1_bias[:, columns]
        hidden = 0.5 * hidden * (1.0 + lax.erf(hidden * math.sqrt(0.5)))
        total[...] += jnp.dot(hidden.astype(BF16), w_fc2[columns, :], preferred_element_type=F32)
    encoded[...] = total[...].astype(BF16)

    def finish(peer):
        sum_copy(me, peer).wait_send()
        for kind in range(3):
            projected_copy(kind, me, peer).wait_send()
        mixed_copy(me, peer).wait_send()

    each_peer(finish)

    @pl.when(me < n - 1)
    def _():
        up.wait_send()

    @pl.when(me > 0)
    def _():
        down.wait_send()


def per_device(
    density,
    stem_weight,
    stem_bias,
    pos_embed,
    ln1_gain,
    ln1_bias,
    w_qkv,
    qkv_bias,
    w_out,
    out_bias,
    ln2_gain,
    ln2_bias,
    w_fc1,
    fc1_bias,
    w_fc2,
    fc2_bias,
):
    n = lax.axis_size("ctx")
    tokens, width = pos_embed.shape
    hidden_width = w_fc1.shape[1]
    planes, side, _ = density.shape
    assert planes == STRIDE and tokens == (side // STRIDE) ** 2
    head_size = width // HEADS
    local_heads = max(HEADS // n, 1)
    groups = max(n // HEADS, 1)
    head_groups = HEADS // local_heads
    group_width = local_heads * head_size
    share = tokens // groups
    pair = 2 * side
    window = planes + 2
    vmem = pl.BlockSpec(memory_space=pltpu.VMEM)
    hbm = pl.BlockSpec(memory_space=pl.ANY)

    def line(vector):
        return vector.reshape(1, -1)

    dma = pltpu.SemaphoreType.DMA
    wide_shape = (n * tokens, 2 * group_width) if group_width % 128 == 0 else (16, 128)
    return pl.pallas_call(
        functools.partial(layer_kernel, n, density.size * n),
        out_shape=jax.ShapeDtypeStruct((tokens, width), BF16),
        in_specs=[
            vmem, vmem, vmem, vmem, vmem, vmem, hbm, vmem,
            hbm, vmem, vmem, vmem, hbm, vmem, hbm, vmem,
        ],
        out_specs=vmem,
        scratch_shapes=[
            pltpu.VMEM(w_qkv.shape, BF16),
            pltpu.VMEM(w_out.shape, BF16),
            pltpu.VMEM(w_fc1.shape, BF16),
            pltpu.VMEM(w_fc2.shape, BF16),
            dma((4,)),
            pltpu.VMEM((2, side, side), F32),
            pltpu.VMEM((8, 128), F32),
            pltpu.VMEM((n, 8, 128), F32),
            dma((2,)),
            dma((2,)),
            dma((n,)),
            dma((n,)),
            pltpu.VMEM((KERNEL, tokens, side), BF16),
            pltpu.VMEM((KERNEL, window * pair, 256), BF16),
            pltpu.VMEM((side, window * pair), BF16),
            pltpu.VMEM((256, width), BF16),
            pltpu.VMEM((tokens, width), BF16),
            pltpu.VMEM((tokens, width), BF16),
            pltpu.VMEM((3, head_groups, tokens, group_width), BF16),
            pltpu.VMEM((n, share, group_width), BF16),
            pltpu.VMEM((n, tokens, group_width), BF16),
            pltpu.VMEM((n, tokens, group_width), BF16),
            pltpu.VMEM(wide_shape, BF16),
            pltpu.VMEM((n, share, group_width), BF16),
            pltpu.VMEM((n, share, group_width), BF16),
            pltpu.VMEM((tokens, width), BF16),
            pltpu.VMEM((tokens, width), F32),
            dma((4, n)),
            dma((4, n)),
        ],
        compiler_params=pltpu.CompilerParams(
            collective_id=0, has_side_effects=True, vmem_limit_bytes=60 * 1024 * 1024
        ),
    )(
        density,
        stem_weight,
        line(stem_bias),
        pos_embed,
        line(ln1_gain),
        line(ln1_bias),
        w_qkv,
        line(qkv_bias),
        w_out,
        line(out_bias),
        line(ln2_gain),
        line(ln2_bias),
        w_fc1,
        line(fc1_bias),
        w_fc2,
        line(fc2_bias),
    )


def solution(mesh):
    in_specs = (P(("dp", "ctx"), None, None), P(), P(), P("ctx", None)) + (P(),) * 12
    return jax.shard_map(
        per_device,
        mesh=mesh,
        in_specs=in_specs,
        out_specs=P(("dp", "ctx"), None),
        check_vma=False,
    )
```

```python
import functools
import math

import jax
import jax.numpy as jnp
from jax import lax
from jax.experimental import pallas as pl
from jax.experimental.pallas import tpu as pltpu
from jax.sharding import PartitionSpec as P

HEADS = 16
KERNEL = 6
STRIDE = 4
ROWS = 128
MESH = pl.DeviceIdType.MESH
F32 = jnp.float32
BF16 = jnp.bfloat16


def iota(shape, axis):
    return lax.broadcasted_iota(jnp.int32, shape, axis)


def partner(me, mask, n):
    result, bit = 0, 1
    while bit < n:
        result += ((me // bit + mask // bit) % 2) * bit
        bit *= 2
    return result


def norm_rows(values, gain_vector, shift_vector):
    center = values - jnp.mean(values, axis=-1, keepdims=True)
    spread = jnp.mean(center * center, axis=-1, keepdims=True)
    return center * lax.rsqrt(spread + 1e-06) * gain_vector + shift_vector


def layer_kernel(
    n,
    cells,
    density,
    stem_weight,
    stem_bias,
    pos_embed,
    ln1_gain,
    ln1_bias,
    w_qkv_hbm,
    qkv_bias,
    w_out_hbm,
    out_bias,
    ln2_gain,
    ln2_bias,
    w_fc1_hbm,
    fc1_bias,
    w_fc2_hbm,
    fc2_bias,
    encoded,
    w_qkv,
    w_out,
    w_fc1,
    w_fc2,
    weight_sem,
    halo,
    sum_send,
    sum_got,
    edge_send_sem,
    edge_recv_sem,
    sum_send_sem,
    sum_recv_sem,
    select_rows,
    fold,
    planes_wide,
    kernel_rows,
    residual,
    normed,
    outgoing,
    query_got,
    key_got,
    value_got,
    value_wide,
    mixed_send,
    mixed_got,
    attended,
    total,
    send_sem,
    recv_sem,
):
    me = lax.axis_index("ctx")
    planes, side, _ = density.shape
    tokens, width = residual.shape
    head_size = width // HEADS
    local_heads = max(HEADS // n, 1)
    groups = max(n // HEADS, 1)
    group_width = local_heads * head_size
    share = tokens // groups
    grid = side // STRIDE
    window = planes + 2

    weights = [
        pltpu.make_async_copy(source, target, weight_sem.at[i])
        for i, (source, target) in enumerate(
            ((w_qkv_hbm, w_qkv), (w_out_hbm, w_out), (w_fc1_hbm, w_fc1), (w_fc2_hbm, w_fc2))
        )
    ]
    for copy in weights:
        copy.start()

    barrier = pltpu.get_barrier_semaphore()

    def each_peer(action):
        def step(offset, carry):
            action(partner(me, n - offset, n))
            return carry

        lax.fori_loop(1, n, step, 0)

    each_peer(
        lambda peer: pl.semaphore_signal(
            barrier, inc=1, device_id={"ctx": peer}, device_id_type=MESH
        )
    )

    own = jnp.sum(density[...], axis=0)
    own = jnp.sum(own, axis=(0, 1), keepdims=True)
    sum_send[...] = jnp.broadcast_to(own, sum_send.shape)
    sum_got[me] = jnp.broadcast_to(own, sum_send.shape)

    @pl.when(me == 0)
    def _():
        halo[0] = jnp.ones((side, side), F32)

    @pl.when(me == n - 1)
    def _():
        halo[1] = jnp.ones((side, side), F32)

    pl.semaphore_wait(barrier, n - 1)

    def edge(side_index, plane, peer):
        return pltpu.make_async_remote_copy(
            src_ref=density.at[plane],
            dst_ref=halo.at[side_index],
            send_sem=edge_send_sem.at[side_index],
            recv_sem=edge_recv_sem.at[side_index],
            device_id={"ctx": peer},
            device_id_type=MESH,
        )

    up = edge(0, planes - 1, lax.rem(me + 1, n))
    down = edge(1, 0, lax.rem(me + n - 1, n))

    def sum_copy(source, peer):
        return pltpu.make_async_remote_copy(
            src_ref=sum_send,
            dst_ref=sum_got.at[source],
            send_sem=sum_send_sem.at[peer],
            recv_sem=sum_recv_sem.at[source],
            device_id={"ctx": peer},
            device_id_type=MESH,
        )

    each_peer(lambda peer: sum_copy(me, peer).start())

    @pl.when(me < n - 1)
    def _():
        up.start()

    @pl.when(me > 0)
    def _():
        down.start()

    pair = 2 * side
    row = iota((tokens, side), 0)
    col = iota((tokens, side), 1)
    for b in range(KERNEL):
        hit = col == STRIDE * (row // grid) - 1 + b
        select_rows[b] = jnp.where(hit, 1.0, 0.0).astype(BF16)
    lane_row = iota((pair, 256), 0)
    lane_col = iota((pair, 256), 1)
    high = lane_row // side
    offset_c = ((lane_row + 1) & (STRIDE - 1)) + STRIDE * high
    for b in range(KERNEL):
        for a in range(window):
            hit = (offset_c < KERNEL) & (lane_col == (a * KERNEL + b) * KERNEL + offset_c)
            fold[b, a * pair : (a + 1) * pair, :] = jnp.where(hit, 1.0, 0.0).astype(BF16)
    taps = stem_weight.shape[0]
    kernel_rows[...] = jnp.zeros(kernel_rows.shape, BF16)
    kernel_rows[0:taps, :] = stem_weight[...]
    tile_row = iota((tokens, pair), 0)
    tile_lane = iota((tokens, pair), 1)
    keep = (((tile_lane & (side - 1)) + 1) // STRIDE - tile_lane // side) == (
        tile_row & (grid - 1)
    )
    keep = jnp.where(keep, 1.0, 0.0).astype(BF16)

    each_peer(lambda peer: sum_copy(peer, peer).wait_recv())

    @pl.when(me > 0)
    def _():
        up.wait_recv()

    @pl.when(me < n - 1)
    def _():
        down.wait_recv()

    mean_density = (jnp.sum(sum_got[...], axis=0)[0:1, 0:1]) / cells
    for a in range(window):
        if a == 0:
            plane = jnp.where(me > 0, jnp.log(halo[0] / mean_density), 0.0)
        elif a == window - 1:
            plane = jnp.where(me < n - 1, jnp.log(halo[1] / mean_density), 0.0)
        else:
            plane = jnp.log(density[a - 1] / mean_density)
        plane = plane.astype(BF16)
        planes_wide[:, a * pair : (a + 1) * pair] = jnp.concatenate([plane, plane], axis=1)

    keep_wide = jnp.concatenate([keep] * window, axis=1)
    patches = jnp.zeros((tokens, 256), F32)
    for b in range(KERNEL):
        rows = jnp.dot(select_rows[b], planes_wide[...], preferred_element_type=F32)
        rows = rows.astype(BF16) * keep_wide
        patches += jnp.dot(rows, fold[b], preferred_element_type=F32)
    embedded = jnp.dot(patches.astype(BF16), kernel_rows[...], preferred_element_type=F32)
    embedded = embedded + stem_bias[...] + pos_embed[...].astype(F32)
    residual[...] = embedded.astype(BF16)
    normed[...] = norm_rows(residual[...].astype(F32), ln1_gain[...], ln1_bias[...]).astype(BF16)

    def head_group(peer):
        return peer // groups

    def my_rows(peer):
        return pl.ds(pl.multiple_of(lax.rem(peer, groups) * share, share), share)

    def projected_copy(kind, source, peer):
        piece = outgoing.at[kind, head_group(peer)]
        got = (query_got, key_got, value_got)[kind]
        if kind == 0:
            piece = piece.at[my_rows(peer)]
        return pltpu.make_async_remote_copy(
            src_ref=piece,
            dst_ref=got.at[source],
            send_sem=send_sem.at[kind, peer],
            recv_sem=recv_sem.at[kind, source],
            device_id={"ctx": peer},
            device_id_type=MESH,
        )

    weights[0].wait()
    block = 256
    for kind in (1, 2, 0):
        for start in range(0, width, block):
            columns = slice(kind * width + start, kind * width + start + block)
            result = jnp.dot(normed[...], w_qkv[:, columns], preferred_element_type=F32)
            result = result + qkv_bias[:, columns]
            if kind == 0:
                result = result * (1.0 / head_size**0.5)
            result = result.astype(BF16)
            for part in range(block // group_width):
                outgoing[kind, start // group_width + part] = result[
                    :, part * group_width : (part + 1) * group_width
                ]
        each_peer(lambda peer: projected_copy(kind, me, peer).start())
    query_got[me] = outgoing[0, head_group(me), my_rows(me), :]
    key_got[me] = outgoing[1, head_group(me)]
    value_got[me] = outgoing[2, head_group(me)]

    each_peer(lambda peer: projected_copy(1, peer, peer).wait_recv())
    each_peer(lambda peer: projected_copy(2, peer, peer).wait_recv())

    keys_total = n * tokens
    wide = group_width % 128 == 0
    if wide:
        value_wide[:, 0:group_width] = value_got[...].reshape(keys_total, group_width)
        value_wide[:, group_width:] = jnp.ones((keys_total, group_width), BF16)

    def mixed_copy(source, peer):
        return pltpu.make_async_remote_copy(
            src_ref=mixed_send.at[peer],
            dst_ref=mixed_got.at[source],
            send_sem=send_sem.at[3, peer],
            recv_sem=recv_sem.at[3, source],
            device_id={"ctx": peer},
            device_id_type=MESH,
        )

    def attend(offset, carry):
        peer = partner(me, lax.rem(n - offset, n), n)

        @pl.when(offset > 0)
        def _():
            projected_copy(0, peer, peer).wait_recv()

        rows = min(share, ROWS)
        for first in range(0, share, rows):
            query = query_got[peer, first : first + rows, :]
            lane = iota((rows, group_width), 1) // head_size
            mixed = None
            for head in range(local_heads):
                mine = query
                if local_heads > 1:
                    mine = jnp.where(lane == head, query, jnp.zeros_like(query))
                scores = lax.dot_general(
                    mine,
                    key_got[...].reshape(keys_total, group_width),
                    (((1,), (1,)), ((), ())),
                    preferred_element_type=F32,
                )
                weight = jnp.exp(scores - jnp.max(scores, axis=1, keepdims=True))
                values = value_wide[...] if wide else value_got[...].reshape(keys_total, group_width)
                product = jnp.dot(weight.astype(BF16), values, preferred_element_type=F32)
                if wide:
                    part = product[:, 0:group_width] / product[:, group_width:]
                else:
                    part = product / jnp.sum(weight, axis=1, keepdims=True)
                mixed = part if mixed is None else jnp.where(lane == head, part, mixed)
            mixed_send[peer, first : first + rows, :] = mixed.astype(BF16)

        @pl.when(offset > 0)
        def _():
            mixed_copy(me, peer).start()

        @pl.when(offset == 0)
        def _():
            mixed_got[me] = mixed_send[me]

        return carry

    lax.fori_loop(0, n, attend, 0)

    each_peer(lambda peer: mixed_copy(peer, peer).wait_recv())
    for piece in range(n):
        first = (piece % groups) * share
        column = (piece // groups) * group_width
        attended[first : first + share, column : column + group_width] = mixed_got[piece]

    weights[1].wait()
    stream = (
        residual[...].astype(F32)
        + jnp.dot(attended[...], w_out[...], preferred_element_type=F32)
        + out_bias[...]
    ).astype(BF16)
    residual[...] = stream
    stream = stream.astype(F32)
    normed[...] = norm_rows(stream, ln2_gain[...], ln2_bias[...]).astype(BF16)
    total[...] = stream + fc2_bias[...]

    weights[2].wait()
    weights[3].wait()
    hidden_width = w_fc1.shape[1]
    tile = math.gcd(hidden_width, 512)
    for start in range(0, hidden_width, tile):
        columns = slice(start, start + tile)
        hidden = jnp.dot(normed[...], w_fc1[:, columns], preferred_element_type=F32)
        hidden = hidden + fc1_bias[:, columns]
        hidden = 0.5 * hidden * (1.0 + lax.erf(hidden * math.sqrt(0.5)))
        total[...] += jnp.dot(hidden.astype(BF16), w_fc2[columns, :], preferred_element_type=F32)
    encoded[...] = total[...].astype(BF16)

    def finish(peer):
        sum_copy(me, peer).wait_send()
        for kind in range(3):
            projected_copy(kind, me, peer).wait_send()
        mixed_copy(me, peer).wait_send()

    each_peer(finish)

    @pl.when(me < n - 1)
    def _():
        up.wait_send()

    @pl.when(me > 0)
    def _():
        down.wait_send()


def per_device(
    density,
    stem_weight,
    stem_bias,
    pos_embed,
    ln1_gain,
    ln1_bias,
    w_qkv,
    qkv_bias,
    w_out,
    out_bias,
    ln2_gain,
    ln2_bias,
    w_fc1,
    fc1_bias,
    w_fc2,
    fc2_bias,
):
    n = lax.axis_size("ctx")
    tokens, width = pos_embed.shape
    hidden_width = w_fc1.shape[1]
    planes, side, _ = density.shape
    assert planes == STRIDE and tokens == (side // STRIDE) ** 2
    head_size = width // HEADS
    local_heads = max(HEADS // n, 1)
    groups = max(n // HEADS, 1)
    head_groups = HEADS // local_heads
    group_width = local_heads * head_size
    share = tokens // groups
    pair = 2 * side
    window = planes + 2
    vmem = pl.BlockSpec(memory_space=pltpu.VMEM)
    hbm = pl.BlockSpec(memory_space=pl.ANY)

    def line(vector):
        return vector.reshape(1, -1)

    dma = pltpu.SemaphoreType.DMA
    wide_shape = (n * tokens, 2 * group_width) if group_width % 128 == 0 else (16, 128)
    return pl.pallas_call(
        functools.partial(layer_kernel, n, density.size * n),
        out_shape=jax.ShapeDtypeStruct((tokens, width), BF16),
        in_specs=[
            vmem, vmem, vmem, vmem, vmem, vmem, hbm, vmem,
            hbm, vmem, vmem, vmem, hbm, vmem, hbm, vmem,
        ],
        out_specs=vmem,
        scratch_shapes=[
            pltpu.VMEM(w_qkv.shape, BF16),
            pltpu.VMEM(w_out.shape, BF16),
            pltpu.VMEM(w_fc1.shape, BF16),
            pltpu.VMEM(w_fc2.shape, BF16),
            dma((4,)),
            pltpu.VMEM((2, side, side), F32),
            pltpu.VMEM((8, 128), F32),
            pltpu.VMEM((n, 8, 128), F32),
            dma((2,)),
            dma((2,)),
            dma((n,)),
            dma((n,)),
            pltpu.VMEM((KERNEL, tokens, side), BF16),
            pltpu.VMEM((KERNEL, window * pair, 256), BF16),
            pltpu.VMEM((side, window * pair), BF16),
            pltpu.VMEM((256, width), BF16),
            pltpu.VMEM((tokens, width), BF16),
            pltpu.VMEM((tokens, width), BF16),
            pltpu.VMEM((3, head_groups, tokens, group_width), BF16),
            pltpu.VMEM((n, share, group_width), BF16),
            pltpu.VMEM((n, tokens, group_width), BF16),
            pltpu.VMEM((n, tokens, group_width), BF16),
            pltpu.VMEM(wide_shape, BF16),
            pltpu.VMEM((n, share, group_width), BF16),
            pltpu.VMEM((n, share, group_width), BF16),
            pltpu.VMEM((tokens, width), BF16),
            pltpu.VMEM((tokens, width), F32),
            dma((4, n)),
            dma((4, n)),
        ],
        compiler_params=pltpu.CompilerParams(
            collective_id=0, has_side_effects=True, vmem_limit_bytes=60 * 1024 * 1024
        ),
    )(
        density,
        stem_weight,
        line(stem_bias),
        pos_embed,
        line(ln1_gain),
        line(ln1_bias),
        w_qkv,
        line(qkv_bias),
        w_out,
        line(out_bias),
        line(ln2_gain),
        line(ln2_bias),
        w_fc1,
        line(fc1_bias),
        w_fc2,
        line(fc2_bias),
    )


def solution(mesh):
    in_specs = (P(("dp", "ctx"), None, None), P(), P(), P("ctx", None)) + (P(),) * 12
    return jax.shard_map(
        per_device,
        mesh=mesh,
        in_specs=in_specs,
        out_specs=P(("dp", "ctx"), None),
        check_vma=False,
    )
```
